8 devices in a mesh: dp: 2 (over z, y), cp: 4 (over x, core).
Axes of the slice: x: 2, y: 2, z: 1, core: 2. Of those that a mesh axis runs over, the one named last changes fastest.
Arguments:
- latents: bfloat16 [32, 64, 64, 16], P('dp', 'cp'), parts along dimension 0
- w_in: bfloat16 [3, 3, 16, 512], replicated
- b_in: bfloat16 [512], replicated
- w_conv: bfloat16 [4, 3, 3, 512, 512], replicated
- b_conv: bfloat16 [4, 512], replicated
- gn_scale: bfloat16 [5, 512], replicated
- gn_shift: bfloat16 [5, 512], replicated
- w_attn: bfloat16 [4, 512, 512], replicated
- b_attn: bfloat16 [4, 512], replicated
Outputs:
- output: bfloat16 [32, 64, 64, 512], P('dp', 'cp'), parts along dimension 0
There are 2 independent parts. The reference program is written for one: setup_inputs(seed, part) draws one part's arguments, and reference() takes and returns one part's arrays. A program takes and returns all parts, laid end to end along the dimension named above; an argument that names none is the same for every part.
All inputs are finite; a program needn't handle non-finite values.
Results may differ from the reference program's by a relative error of at most 0.0157452.
Values are sent between devices in bfloat16 or wider.
A program may use at most 1 GiB of HBM per device.

```python
import jax
import jax.numpy as jnp
from jax import lax

SAMPLES = 16
LAT_H = 64
LAT_W = 64
Z_CH = 16
CHANNELS = 512
GROUPS = 32
QUERY_TOKENS = 1024
GN_EPS = 1e-6


def setup_inputs(seed: int = 0, part: int = 0) -> dict:
    root_key = jax.random.key(seed)
    rand_keys = jax.random.split(root_key, 9)
    lat_keys = jax.random.split(jax.random.fold_in(rand_keys[0], part), 4)
    lat_noise = jax.random.normal(lat_keys[0], (SAMPLES, LAT_H, LAT_W, Z_CH), jnp.float32)
    row_pos = (2.0 * jnp.arange(LAT_H, dtype=jnp.float32) / (LAT_H - 1) - 1.0).reshape(1, LAT_H, 1, 1)
    row_slope = 0.8 * jax.random.normal(lat_keys[1], (SAMPLES, 1, 1, Z_CH), jnp.float32)
    row_scale = jax.random.uniform(lat_keys[2], (SAMPLES, LAT_H, 1, 1), jnp.float32, 0.6, 1.4)
    row_shift = 0.3 * jax.random.normal(lat_keys[3], (SAMPLES, LAT_H, 1, Z_CH), jnp.float32)
    latents = lat_noise * row_scale + row_slope * row_pos + row_shift
    attn_gain = jnp.array([2.4, 2.4, 1.0, 1.0], dtype=jnp.float32).reshape(4, 1, 1)
    w_in = jax.random.normal(rand_keys[1], (3, 3, Z_CH, CHANNELS), jnp.float32) * (9 * Z_CH) ** -0.5
    b_in = 0.5 * jax.random.normal(rand_keys[2], (CHANNELS,), jnp.float32)
    w_conv = jax.random.normal(rand_keys[3], (4, 3, 3, CHANNELS, CHANNELS), jnp.float32) * (9 * CHANNELS) ** -0.5
    b_conv = 0.3 * jax.random.normal(rand_keys[4], (4, CHANNELS), jnp.float32)
    gn_scale = 1.0 + 0.3 * jax.random.normal(rand_keys[5], (5, CHANNELS), jnp.float32)
    gn_shift = 0.3 * jax.random.normal(rand_keys[6], (5, CHANNELS), jnp.float32)
    w_attn = jax.random.normal(rand_keys[7], (4, CHANNELS, CHANNELS), jnp.float32) * attn_gain * CHANNELS ** -0.5
    b_attn = 0.3 * jax.random.normal(rand_keys[8], (4, CHANNELS), jnp.float32)
    return {
        'latents': latents.astype(jnp.bfloat16),
        'w_in': w_in.astype(jnp.bfloat16),
        'b_in': b_in.astype(jnp.bfloat16),
        'w_conv': w_conv.astype(jnp.bfloat16),
        'b_conv': b_conv.astype(jnp.bfloat16),
        'gn_scale': gn_scale.astype(jnp.bfloat16),
        'gn_shift': gn_shift.astype(jnp.bfloat16),
        'w_attn': w_attn.astype(jnp.bfloat16),
        'b_attn': b_attn.astype(jnp.bfloat16),
    }


def conv3x3(x_val, weight, conv_bias):
    conv_out = lax.conv_general_dilated(x_val.astype(jnp.float32), weight.astype(jnp.float32), (1, 1), 'SAME', dimension_numbers=('NHWC', 'HWIO', 'NHWC'))
    return conv_out + conv_bias.astype(jnp.float32)


def group_norm(x_val, norm_gain, norm_bias):
    n_batch, n_rows, n_width, n_chan = x_val.shape
    grouped = x_val.astype(jnp.float32).reshape(n_batch, n_rows, n_width, GROUPS, n_chan // GROUPS)
    grp_mean = jnp.mean(grouped, axis=(1, 2, 4), keepdims=True)
    centered = grouped - grp_mean
    grp_var = jnp.mean(jnp.square(centered), axis=(1, 2, 4), keepdims=True)
    normed = (centered * lax.rsqrt(grp_var + GN_EPS)).reshape(x_val.shape)
    return normed * norm_gain.astype(jnp.float32) + norm_bias.astype(jnp.float32)


def resnet_block(h_val, w_conv, b_conv, gn_scale, gn_shift, conv_idx, norm_idx):
    act_in = jax.nn.silu(group_norm(h_val, gn_scale[norm_idx], gn_shift[norm_idx])).astype(jnp.bfloat16)
    mid_act = conv3x3(act_in, w_conv[conv_idx], b_conv[conv_idx]).astype(jnp.bfloat16)
    act_two = jax.nn.silu(group_norm(mid_act, gn_scale[norm_idx + 1], gn_shift[norm_idx + 1])).astype(jnp.bfloat16)
    conv_two = conv3x3(act_two, w_conv[conv_idx + 1], b_conv[conv_idx + 1])
    return (h_val.astype(jnp.float32) + conv_two).astype(jnp.bfloat16)


def attention(h_val, w_attn, b_attn, norm_gain, norm_bias):
    n_batch, n_rows, n_width, n_chan = h_val.shape
    normed = group_norm(h_val, norm_gain, norm_bias).astype(jnp.bfloat16).reshape(-1, n_chan)

    def project(j_idx):
        proj = jnp.dot(normed, w_attn[j_idx], preferred_element_type=jnp.float32) + b_attn[j_idx].astype(jnp.float32)
        return proj.astype(jnp.bfloat16).reshape(n_batch, n_rows * n_width, n_chan)

    queries = project(0)
    keys_all = project(1)
    vals_all = project(2)
    block_rows = max([divisor for divisor in range(1, n_rows + 1) if n_rows % divisor == 0 and divisor * n_width <= QUERY_TOKENS] + [1])
    n_blocks = n_rows // block_rows
    att_scale = n_chan ** -0.5

    def one_sample(operands):
        q_sample, k_sample, v_sample = operands

        def one_block(q_block):
            scores = jnp.dot(q_block, k_sample.T, preferred_element_type=jnp.float32) * att_scale
            attn_prob = jax.nn.softmax(scores, axis=-1).astype(jnp.bfloat16)
            return jnp.dot(attn_prob, v_sample, preferred_element_type=jnp.float32).astype(jnp.bfloat16)

        return lax.map(one_block, q_sample.reshape(n_blocks, block_rows * n_width, n_chan))

    attended = lax.map(one_sample, (queries, keys_all, vals_all)).reshape(-1, n_chan)
    proj_out = jnp.dot(attended, w_attn[3], preferred_element_type=jnp.float32) + b_attn[3].astype(jnp.float32)
    return (h_val.astype(jnp.float32) + proj_out.reshape(h_val.shape)).astype(jnp.bfloat16)


def reference(latents, w_in, b_in, w_conv, b_conv, gn_scale, gn_shift, w_attn, b_attn):
    hidden = conv3x3(latents, w_in, b_in).astype(jnp.bfloat16)
    hidden = resnet_block(hidden, w_conv, b_conv, gn_scale, gn_shift, 0, 0)
    hidden = attention(hidden, w_attn, b_attn, gn_scale[2], gn_shift[2])
    hidden = resnet_block(hidden, w_conv, b_conv, gn_scale, gn_shift, 2, 3)
    return hidden
```

```python
import functools

import jax
import jax.numpy as jnp
import numpy as np
from jax import lax
from jax.experimental import pallas as pl
from jax.experimental.pallas import tpu as pltpu
from jax.sharding import PartitionSpec as P

GROUPS = 32
GN_EPS = 1e-6
LANES = 128
BLOCK_ROWS = 8
F32 = jnp.float32
BF16 = jnp.bfloat16


def sample_kernel(me_ref, x_hbm, w_in_ref, b_in_ref, w_conv_hbm, b_conv_ref, gn_scale_ref, gn_shift_ref,
                  w_attn_hbm, b_attn_ref, b_key_ref, *rest):
    n_dev = len(rest) - 15
    outs = rest[:n_dev]
    (w_conv, w_attn, h, t, kt, v, buf_a, buf_b, s_buf, p_buf, o_buf, m_buf, l_buf, small, sems) = rest[n_dev:]
    n_rows, width, chan = h.shape
    tokens = n_rows * width
    blk = BLOCK_ROWS * width
    n_blk = n_rows // BLOCK_ROWS
    depth = 3 * chan
    count = tokens * (chan // GROUPS)
    n_cols = w_in_ref.shape[0]
    stat, coef = small.at[0:2], small.at[2:4]
    acc_a, acc_b = s_buf.at[:, 0:chan], s_buf.at[:, chan:2 * chan]
    def conv_copy(idx):
        return pltpu.make_async_copy(w_conv_hbm.at[idx], w_conv.at[idx], sems.at[idx])

    attn_copy = pltpu.make_async_copy(w_attn_hbm, w_attn, sems.at[4])
    x_copy = pltpu.make_async_copy(x_hbm.at[me_ref[1]], p_buf.at[0:n_cols, :], sems.at[5])
    x_copy.start()
    conv_copy(0).start()
    conv_copy(1).start()
    attn_copy.start()
    conv_copy(2).start()
    conv_copy(3).start()

    def zero_stats():
        stat[...] = jnp.zeros((2, 8, chan), F32)

    def finish(get, put, live):
        for col in range(0, chan, LANES):
            tot = jnp.zeros((8, LANES), F32)
            tot_sq = jnp.zeros((8, LANES), F32)
            for r in range(BLOCK_ROWS):
                val = get(r, col).astype(BF16)
                put(r, col, val)
                val = val.astype(F32).reshape(width // 8, 8, LANES)
                tot = tot + jnp.sum(val, axis=0)
                tot_sq = tot_sq + jnp.sum(val * val, axis=0)
            if live is not None:
                tot = jnp.where(live, tot, 0.0)
                tot_sq = jnp.where(live, tot_sq, 0.0)
            stat[0, :, col:col + LANES] += tot
            stat[1, :, col:col + LANES] += tot_sq

    def set_coefs(idx, half):
        lane = lax.broadcasted_iota(jnp.int32, (8, chan), 1)

        def group_sum(part):
            tot = jnp.broadcast_to(jnp.sum(part, axis=0, keepdims=True), (8, chan))
            for step in (1, 2, 4, 8):
                above = pltpu.roll(tot, chan - step, 1)
                below = pltpu.roll(tot, step, 1)
                tot = tot + jnp.where((lane & step) == 0, above, below)
            return tot

        mean = group_sum(stat[0]) * (1.0 / count)
        var = jnp.maximum(group_sum(stat[1]) * (1.0 / count) - mean * mean, 0.0)
        gain = gn_scale_ref[idx] * lax.rsqrt(var + GN_EPS)
        shift = gn_shift_ref[idx] - mean * gain
        coef[0] = gain * half
        coef[1] = shift * half

    zero_stats()

    def conv_in_step(b, carry):
        lhs = p_buf[0:n_cols, pl.ds(pl.multiple_of(b * blk, blk), blk)]
        acc_a[...] = lax.dot_general(lhs, w_in_ref[...], (((0,), (0,)), ((), ())), preferred_element_type=F32)

        def get(r, col):
            return acc_a[r * width:(r + 1) * width, col:col + LANES] + b_in_ref[0:1, col:col + LANES]

        def put(r, col, val):
            h[b * BLOCK_ROWS + r, :, col:col + LANES] = val

        finish(get, put, None)
        return carry

    x_copy.wait()
    lax.fori_loop(0, n_blk, conv_in_step, 0)

    def prep(src, buf, b):
        col_pos = lax.broadcasted_iota(jnp.int32, (width, LANES), 0)
        for r in range(BLOCK_ROWS + 2):
            row = b * BLOCK_ROWS + (r - 1)
            row_c = jnp.clip(row, 0, n_rows - 1)
            for col in range(0, chan, LANES):
                gain = coef[0, 0:1, col:col + LANES]
                shift = coef[1, 0:1, col:col + LANES]
                z = src[row_c, :, col:col + LANES].astype(F32) * gain + shift
                u = z + z * jnp.tanh(z)
                if r in (0, BLOCK_ROWS + 1):
                    u = jnp.where((row >= 0) & (row < n_rows), u, 0.0)
                left = jnp.where(col_pos == 0, 0.0, pltpu.roll(u, 1, 0))
                right = jnp.where(col_pos == width - 1, 0.0, pltpu.roll(u, width - 1, 0))
                buf[r, :, col:col + LANES] = left.astype(BF16)
                buf[r, :, chan + col:chan + col + LANES] = u.astype(BF16)
                buf[r, :, 2 * chan + col:2 * chan + col + LANES] = right.astype(BF16)

    def conv_dots(buf, acc, idx):
        tot = None
        for dy in range(3):
            lhs = buf[dy:dy + BLOCK_ROWS].reshape(blk, depth)
            part = jnp.dot(lhs, w_conv[idx, dy * depth:(dy + 1) * depth, :], preferred_element_type=F32)
            tot = part if tot is None else tot + part
        acc[...] = tot

    def conv_finish(acc, dst, idx, b, residual, live):
        row0 = jnp.maximum(b, 0) * BLOCK_ROWS

        def get(r, col):
            val = acc[r * width:(r + 1) * width, col:col + LANES] + b_conv_ref[idx, 0:1, col:col + LANES]
            if residual:
                old = dst[row0 + r, :, col:col + LANES].astype(F32)
                val = old + val
                if live is not None:
                    val = jnp.where(live, val, old)
            return val

        def put(r, col, val):
            dst[row0 + r, :, col:col + LANES] = val

        finish(get, put, live)

    def conv_pass(src, dst, idx, residual):
        zero_stats()
        prep(src, buf_a, 0)
        conv_copy(idx).wait()

        def pair(j, carry):
            conv_dots(buf_a, acc_a, idx)
            prep(src, buf_b, 2 * j + 1)
            conv_finish(acc_b, dst, idx, 2 * j - 1, residual, j > 0)
            conv_dots(buf_b, acc_b, idx)
            prep(src, buf_a, 2 * j + 2)
            conv_finish(acc_a, dst, idx, 2 * j, residual, None)
            return carry

        lax.fori_loop(0, n_blk // 2, pair, 0)
        conv_finish(acc_b, dst, idx, n_blk - 1, residual, None)

    q = t.reshape(tokens, chan)
    kv_chunk = 512
    n_chunk = tokens // kv_chunk
    exp_scale = float(chan ** -0.5 * np.log2(np.e))

    def project(b, carry):
        norm = h[pl.ds(b * BLOCK_ROWS, BLOCK_ROWS)].reshape(blk, chan).astype(F32) * coef[0, 0:1, :] + coef[1, 0:1, :]
        norm = norm.astype(BF16)
        rows = pl.ds(pl.multiple_of(b * blk, blk), blk)
        q[rows, :] = (jnp.dot(norm, w_attn[0], preferred_element_type=F32) + b_attn_ref[0]).astype(BF16)
        v[rows, :] = (jnp.dot(norm, w_attn[2], preferred_element_type=F32) + b_attn_ref[2]).astype(BF16)
        keys = lax.dot_general(w_attn[1], norm, (((1,), (1,)), ((), ())), preferred_element_type=F32)
        kt[:, pl.ds(pl.multiple_of(b * blk, blk), blk)] = (keys + b_key_ref[...]).astype(BF16)
        return carry

    def score_chunk(q_val, c):
        val = jnp.dot(q_val, kt[:, c * kv_chunk:(c + 1) * kv_chunk], preferred_element_type=F32)
        s_buf[:, c * kv_chunk:(c + 1) * kv_chunk] = val
        for r in range(BLOCK_ROWS):
            rows = slice(r * width, (r + 1) * width)
            top = val[rows, 0:LANES]
            for col in range(LANES, kv_chunk, LANES):
                top = jnp.maximum(top, val[rows, col:col + LANES])
            m_buf[0, rows, :] = top if c == 0 else jnp.maximum(m_buf[0, rows, :], top)

    def prob_chunk(c):
        for r in range(BLOCK_ROWS):
            rows = slice(r * width, (r + 1) * width)
            m_scaled = m_buf[1, rows, :]
            tot = None
            for col in range(c * kv_chunk, (c + 1) * kv_chunk, LANES):
                val = jnp.exp2(s_buf[rows, col:col + LANES] * exp_scale - m_scaled)
                p_buf[rows, col:col + LANES] = val.astype(BF16)
                tot = val if tot is None else tot + val
            l_buf[rows, :] = tot if c == 0 else l_buf[rows, :] + tot

    def out_project(b, live):
        row0 = jnp.maximum(b, 0) * BLOCK_ROWS
        prod = jnp.dot(o_buf[...], w_attn[3], preferred_element_type=F32)

        def get(r, col):
            old = h[row0 + r, :, col:col + LANES].astype(F32)
            val = old + (prod[r * width:(r + 1) * width, col:col + LANES] + b_attn_ref[3, 0:1, col:col + LANES])
            return val if live is None else jnp.where(live, val, old)

        def put(r, col, val):
            h[row0 + r, :, col:col + LANES] = val

        finish(get, put, live)

    def score_block(i):
        q_val = q[pl.ds(pl.multiple_of(i * blk, blk), blk), :]
        for c in range(n_chunk):
            score_chunk(q_val, c)
        for r in range(BLOCK_ROWS):
            rows = slice(r * width, (r + 1) * width)
            top = jnp.max(m_buf[0, rows, :], axis=1, keepdims=True) * exp_scale
            m_buf[1, rows, :] = jnp.broadcast_to(top, (width, LANES))

    def weigh_block(more):
        for r in range(BLOCK_ROWS):
            rows = slice(r * width, (r + 1) * width)
            inv = 1.0 / jnp.sum(l_buf[rows, :], axis=1, keepdims=True)
            m_buf[0, rows, :] = jnp.broadcast_to(inv, (width, LANES))
        tot = None
        for c in range(n_chunk):
            cols = slice(c * kv_chunk, (c + 1) * kv_chunk)
            part = jnp.dot(p_buf[:, cols], v[cols, :], preferred_element_type=F32)
            tot = part if tot is None else tot + part
            if more:
                prob_chunk(c)
        for r in range(BLOCK_ROWS):
            rows = slice(r * width, (r + 1) * width)
            for col in range(0, chan, LANES):
                o_buf[rows, col:col + LANES] = (tot[rows, col:col + LANES] * m_buf[0, rows, :]).astype(BF16)

    def attention():
        attn_copy.wait()
        lax.fori_loop(0, n_blk, project, 0)
        zero_stats()
        o_buf[...] = jnp.zeros_like(o_buf)
        score_block(0)

        @pl.when(me_ref[0] >= 0)
        def _():
            for c in range(n_chunk):
                prob_chunk(c)

        def step(i, carry):
            @pl.when(me_ref[0] >= 0)
            def _():
                score_block(i + 1)
                out_project(i - 1, i > 0)

            weigh_block(True)
            return carry

        lax.fori_loop(0, n_blk - 1, step, 0)
        out_project(n_blk - 2, None)
        weigh_block(False)
        out_project(n_blk - 1, None)

    def stage(r, carry):
        set_coefs(3 * r, 0.5)
        conv_pass(h, t, 2 * r, False)
        set_coefs(3 * r + 1, 0.5)
        conv_pass(t, h, 2 * r + 1, True)

        @pl.when(r == 0)
        def _():
            set_coefs(2, 1.0)
            attention()

        return carry

    lax.fori_loop(0, 2, stage, 0)

    me = me_ref[0]
    band = n_rows // n_dev
    copies = [pltpu.make_async_copy(h.at[pl.ds(lax.rem(me + d, n_dev) * band, band)], outs[d], sems.at[d]) for d in range(n_dev)]
    for copy in copies:
        copy.start()
    for copy in copies:
        copy.wait()


def run_sample(me, x, w_in, b_in, w_conv, b_conv, gn_scale, gn_shift, w_attn, b_attn, b_key, n_dev, n_rows, width):
    chan = w_in.shape[1]
    tokens = n_rows * width
    blk = BLOCK_ROWS * width
    vmem = pl.BlockSpec(memory_space=pltpu.VMEM)
    hbm = pl.BlockSpec(memory_space=pl.ANY)
    flops = 2 * tokens * (4 * 9 * chan * chan + 4 * chan * chan + 2 * tokens * chan)
    return pl.pallas_call(
        sample_kernel,
        out_shape=[jax.ShapeDtypeStruct((n_rows // n_dev, width, chan), BF16)] * n_dev,
        in_specs=[pl.BlockSpec(memory_space=pltpu.SMEM), hbm, vmem, vmem, hbm, vmem, vmem, vmem, hbm, vmem, vmem],
        out_specs=[hbm] * n_dev,
        scratch_shapes=[
            pltpu.VMEM(w_conv.shape, BF16),
            pltpu.VMEM(w_attn.shape, BF16),
            pltpu.VMEM((n_rows, width, chan), BF16),
            pltpu.VMEM((n_rows, width, chan), BF16),
            pltpu.VMEM((chan, tokens), BF16),
            pltpu.VMEM((tokens, chan), BF16),
            pltpu.VMEM((BLOCK_ROWS + 2, width, 3 * chan), BF16),
            pltpu.VMEM((BLOCK_ROWS + 2, width, 3 * chan), BF16),
            pltpu.VMEM((blk, tokens), F32),
            pltpu.VMEM((blk, tokens), BF16),
            pltpu.VMEM((blk, chan), BF16),
            pltpu.VMEM((2, blk, LANES), F32),
            pltpu.VMEM((blk, LANES), F32),
            pltpu.VMEM((4, 8, chan), F32),
            pltpu.SemaphoreType.DMA((6,)),
        ],
        compiler_params=pltpu.CompilerParams(vmem_limit_bytes=67_043_328),
        cost_estimate=pl.CostEstimate(flops=flops, bytes_accessed=40 << 20, transcendentals=tokens * tokens),
        name='sample_block',
    )(me, x, w_in, b_in, w_conv, b_conv, gn_scale, gn_shift, w_attn, b_attn, b_key)


def place_kernel(first, n_samples, n_dev, aliased, me_ref, *rest):
    n_in = n_samples * n_dev
    pieces = rest[:n_in]
    out, stage, in_sems, out_sems = rest[n_in + (1 if aliased else 0):]
    per_dev = out.shape[0] // n_dev
    me = me_ref[0]
    loads, stores = [], []
    for i, piece in enumerate(pieces):
        s, d = divmod(i, n_dev)
        owner = lax.rem(me - d + n_dev, n_dev)
        loads.append(pltpu.make_async_copy(piece, stage.at[i], in_sems.at[i]))
        stores.append(pltpu.make_async_copy(stage.at[i], out.at[owner * per_dev + (first + s)], out_sems.at[i]))
    for load in loads:
        load.start()
    for load, store in zip(loads, stores):
        load.wait()
        store.start()
    for store in stores:
        store.wait()


def place(me, pieces, first, n_dev, out_shape, base):
    n_samples = len(pieces) // n_dev
    hbm = pl.BlockSpec(memory_space=pl.ANY)
    args = [me] + list(pieces) + ([] if base is None else [base])
    n_in = len(pieces)
    return pl.pallas_call(
        functools.partial(place_kernel, first, n_samples, n_dev, base is not None),
        out_shape=jax.ShapeDtypeStruct(out_shape, BF16),
        in_specs=[pl.BlockSpec(memory_space=pltpu.SMEM)] + [hbm] * (len(args) - 1),
        out_specs=hbm,
        input_output_aliases={} if base is None else {len(args) - 1: 0},
        scratch_shapes=[
            pltpu.VMEM((n_in,) + tuple(pieces[0].shape), BF16),
            pltpu.SemaphoreType.DMA((n_in,)),
            pltpu.SemaphoreType.DMA((n_in,)),
        ],
        cost_estimate=pl.CostEstimate(flops=1 << 20, bytes_accessed=n_in << 21, transcendentals=0),
        name='place_bands',
    )(*args)


def solution(mesh):
    n_dev = mesh.shape['cp']

    def local_fn(latents, w_in, b_in, w_conv, b_conv, gn_scale, gn_shift, w_attn, b_attn):
        me = lax.axis_index('cp').astype(jnp.int32).reshape(1)
        lat = lax.all_to_all(latents, 'cp', split_axis=0, concat_axis=1, tiled=True)
        n_own, n_rows, width, n_lat = lat.shape
        chan = w_in.shape[-1]
        tokens = n_rows * width
        flat = jnp.transpose(lat.reshape(n_own, tokens, n_lat), (0, 2, 1))
        flat = jnp.pad(flat, ((0, 0), (0, 0), (width + 1, width + 1)))
        col_pos = lax.broadcasted_iota(jnp.int32, (1, 1, tokens), 2) % width
        taps = []
        for dy in range(3):
            for dx in range(3):
                tap = flat[:, :, dy * width + dx:dy * width + dx + tokens]
                if dx == 0:
                    tap = jnp.where(col_pos == 0, jnp.zeros_like(tap), tap)
                if dx == 2:
                    tap = jnp.where(col_pos == width - 1, jnp.zeros_like(tap), tap)
                taps.append(tap)
        cols = jnp.concatenate(taps, axis=1)
        w_in2 = w_in.reshape(9 * n_lat, chan)
        w_conv2 = w_conv.reshape(4, 9 * chan, chan)
        w_attn2 = jnp.stack([w_attn[0], w_attn[1].T, w_attn[2], w_attn[3]])
        out_shape = (n_own * n_dev, n_rows // n_dev, width, chan)

        def rows_of(val):
            return val.astype(F32).reshape(val.shape[:-1] + (1, chan))

        pieces = []
        for s in range(n_own):
            bands = run_sample(jnp.concatenate([me, jnp.full((1,), s, jnp.int32)]), cols, w_in2, rows_of(b_in), w_conv2, rows_of(b_conv), rows_of(gn_scale),
                               rows_of(gn_shift), w_attn2, rows_of(b_attn), b_attn[1].astype(F32).reshape(chan, 1),
                               n_dev, n_rows, width)
            got = [bands[0]]
            for d in range(1, n_dev):
                got.append(lax.ppermute(bands[d], 'cp', [(j, (j + d) % n_dev) for j in range(n_dev)]))
            pieces.append(got)
        early = [piece for got in pieces[:-1] for piece in got]
        out = place(me, early, 0, n_dev, out_shape, None)
        return place(me, pieces[-1], n_own - 1, n_dev, out_shape, out)

    band_spec = P('dp', 'cp')
    whole_spec = P()
    return jax.shard_map(local_fn, mesh=mesh, in_specs=(band_spec,) + (whole_spec,) * 8, out_specs=band_spec, check_vma=False)
```

```python
import functools

import jax
import jax.numpy as jnp
import numpy as np
from jax import lax
from jax.experimental import pallas as pl
from jax.experimental.pallas import tpu as pltpu
from jax.sharding import PartitionSpec as P


GROUPS = 32
GN_EPS = 1e-6
LANES = 128
BLOCK_ROWS = 8
F32 = jnp.float32
BF16 = jnp.bfloat16


def sample_kernel(sample, me_ref, x_hbm, w_in_ref, b_in_ref, w_conv_hbm, b_conv_ref, gn_scale_ref, gn_shift_ref,
                  w_attn_hbm, w_key_hbm, b_attn_ref, b_key_ref, far_out, cross_out, t_out, h_out, coef_out,
                  w_conv, w_attn, h, t, kt, v, s_buf, p_buf, o_buf, o_raw, m_buf, l_buf, small, params, sems):
    n_dev = h.shape[0] // far_out.shape[0]
    n_rows, width, chan = h.shape
    tokens = n_rows * width
    blk = BLOCK_ROWS * width
    n_blk = n_rows // BLOCK_ROWS
    count = tokens * (chan // GROUPS)
    n_cols = w_in_ref.shape[0]
    stat, coef = small.at[0:2], small.at[2:4]
    acc_a, acc_b = s_buf.at[:, 0:chan], s_buf.at[:, chan:2 * chan]
    lhs_rows = 3 * (BLOCK_ROWS + 2) * width
    buf_a, buf_b = v.at[0:lhs_rows], v.at[tokens // 2:tokens // 2 + lhs_rows]

    def conv_copy(idx):
        return pltpu.make_async_copy(w_conv_hbm.at[idx], w_conv.at[idx], sems.at[idx])

    attn_copies = [pltpu.make_async_copy(w_key_hbm if i == 1 else w_attn_hbm.at[i], w_attn.at[i], sems.at[6 + i]) for i in range(4)]
    me = me_ref[0]
    band = n_rows // n_dev
    half = n_rows // 2
    own_row = (me // (n_dev // 2)) * half
    far_row = half - own_row
    for i, ref in enumerate((gn_scale_ref, gn_shift_ref, b_conv_ref, b_attn_ref)):
        val = ref[...].astype(F32)
        for k in range(val.shape[0]):
            params[i, k] = val[k:k + 1]
    gn_scale, gn_shift, b_conv, b_attn = (params.at[i] for i in range(4))
    x_copy = pltpu.make_async_copy(x_hbm.at[sample], p_buf.at[0:n_cols, :], sems.at[5])
    x_copy.start()
    conv_copy(0).start()
    conv_copy(1).start()
    for copy in attn_copies:
        copy.start()
    conv_copy(2).start()
    conv_copy(3).start()

    def zero_stats():
        stat[...] = jnp.zeros((2, 8, chan), F32)

    def finish(get, put, live):
        for col in range(0, chan, LANES):
            tot = jnp.zeros((8, LANES), F32)
            tot_sq = jnp.zeros((8, LANES), F32)
            for r in range(BLOCK_ROWS):
                val = get(r, col).astype(BF16)
                put(r, col, val)
                val = val.astype(F32).reshape(width // 8, 8, LANES)
                tot = tot + jnp.sum(val, axis=0)
                tot_sq = tot_sq + jnp.sum(val * val, axis=0)
            if live is not None:
                tot = jnp.where(live, tot, 0.0)
                tot_sq = jnp.where(live, tot_sq, 0.0)
            stat[0, :, col:col + LANES] += tot
            stat[1, :, col:col + LANES] += tot_sq

    def set_coefs(idx, half):
        lane = lax.broadcasted_iota(jnp.int32, (8, chan), 1)

        def group_sum(part):
            tot = jnp.broadcast_to(jnp.sum(part, axis=0, keepdims=True), (8, chan))
            for step in (1, 2, 4, 8):
                above = pltpu.roll(tot, chan - step, 1)
                below = pltpu.roll(tot, step, 1)
                tot = tot + jnp.where((lane & step) == 0, above, below)
            return tot

        mean = group_sum(stat[0]) * (1.0 / count)
        var = jnp.maximum(group_sum(stat[1]) * (1.0 / count) - mean * mean, 0.0)
        gain = gn_scale[idx] * lax.rsqrt(var + GN_EPS)
        shift = gn_shift[idx] - mean * gain
        coef[0] = gain * half
        coef[1] = shift * half

    zero_stats()

    def conv_in_step(b, carry):
        lhs = p_buf[0:n_cols, pl.ds(pl.multiple_of(b * blk, blk), blk)]
        acc_a[...] = lax.dot_general(lhs, w_in_ref[...], (((0,), (0,)), ((), ())), preferred_element_type=F32)

        def get(r, col):
            return acc_a[r * width:(r + 1) * width, col:col + LANES] + b_in_ref[0:1, col:col + LANES]

        def put(r, col, val):
            h[b * BLOCK_ROWS + r, :, col:col + LANES] = val

        finish(get, put, None)
        return carry

    x_copy.wait()
    lax.fori_loop(0, n_blk, conv_in_step, 0)

    def prep(src, buf, b, base):
        for r in range(BLOCK_ROWS + 2):
            row = base + b * BLOCK_ROWS + (r - 1)
            row_c = jnp.clip(row, 0, n_rows - 1)
            live = (row >= 0) & (row < n_rows) if r in (0, BLOCK_ROWS + 1) else None
            activate_row(src, row_c, coef, buf, r, live)

    def conv_dots(buf, acc, idx):
        dots_of(buf, w_conv.at[idx], acc)

    def conv_finish(acc, dst, idx, b, base, residual, live):
        row0 = base + jnp.maximum(b, 0) * BLOCK_ROWS

        def get(r, col):
            val = acc[r * width:(r + 1) * width, col:col + LANES] + b_conv[idx, 0:1, col:col + LANES]
            if residual:
                old = dst[row0 + r, :, col:col + LANES].astype(F32)
                val = old + val
                if live is not None:
                    val = jnp.where(live, val, old)
            return val

        def put(r, col, val):
            dst[row0 + r, :, col:col + LANES] = val

        finish(get, put, live)

    def conv_pass(src, dst, idx, residual, base, pairs):
        zero_stats()
        prep(src, buf_a, 0, base)
        conv_copy(idx).wait()

        def pair(j, carry):
            conv_dots(buf_a, acc_a, idx)
            prep(src, buf_b, 2 * j + 1, base)
            conv_finish(acc_b, dst, idx, 2 * j - 1, base, residual, j > 0)
            conv_dots(buf_b, acc_b, idx)
            prep(src, buf_a, 2 * j + 2, base)
            conv_finish(acc_a, dst, idx, 2 * j, base, residual, None)
            return carry

        lax.fori_loop(0, pairs, pair, 0)
        conv_finish(acc_b, dst, idx, 2 * pairs - 1, base, residual, None)

    q = t.reshape(tokens, chan)
    kv_chunk = 512
    n_chunk = tokens // kv_chunk
    exp_scale = float(chan ** -0.5 * np.log2(np.e))

    def project(b, carry):
        norm = h[pl.ds(b * BLOCK_ROWS, BLOCK_ROWS)].reshape(blk, chan).astype(F32) * coef[0, 0:1, :] + coef[1, 0:1, :]
        norm = norm.astype(BF16)
        rows = pl.ds(pl.multiple_of(b * blk, blk), blk)
        q[rows, :] = (jnp.dot(norm, w_attn[0], preferred_element_type=F32) + b_attn[0]).astype(BF16)
        v[rows, :] = (jnp.dot(norm, w_attn[2], preferred_element_type=F32) + b_attn[2]).astype(BF16)
        keys = lax.dot_general(w_attn[1], norm, (((1,), (1,)), ((), ())), preferred_element_type=F32)
        kt[:, pl.ds(pl.multiple_of(b * blk, blk), blk)] = (keys + b_key_ref[...]).astype(BF16)
        return carry

    def score_chunk(q_val, c):
        val = jnp.dot(q_val, kt[:, c * kv_chunk:(c + 1) * kv_chunk], preferred_element_type=F32)
        s_buf[:, c * kv_chunk:(c + 1) * kv_chunk] = val
        for r in range(BLOCK_ROWS):
            rows = slice(r * width, (r + 1) * width)
            top = val[rows, 0:LANES]
            for col in range(LANES, kv_chunk, LANES):
                top = jnp.maximum(top, val[rows, col:col + LANES])
            m_buf[0, rows, :] = top if c == 0 else jnp.maximum(m_buf[0, rows, :], top)

    def prob_chunk(c):
        for r in range(BLOCK_ROWS):
            rows = slice(r * width, (r + 1) * width)
            m_scaled = m_buf[1, rows, :]
            tot = None
            for col in range(c * kv_chunk, (c + 1) * kv_chunk, LANES):
                val = jnp.exp2(s_buf[rows, col:col + LANES] * exp_scale - m_scaled)
                p_buf[rows, col:col + LANES] = val.astype(BF16)
                tot = val if tot is None else tot + val
            l_buf[rows, :] = tot if c == 0 else l_buf[rows, :] + tot

    def out_project(b, live):
        row0 = jnp.maximum(b, 0) * BLOCK_ROWS
        prod = jnp.dot(o_buf[...], w_attn[3], preferred_element_type=F32)

        def get(r, col):
            old = h[row0 + r, :, col:col + LANES].astype(F32)
            val = old + (prod[r * width:(r + 1) * width, col:col + LANES] + b_attn[3, 0:1, col:col + LANES])
            return val if live is None else jnp.where(live, val, old)

        def put(r, col, val):
            h[row0 + r, :, col:col + LANES] = val

        finish(get, put, live)

    def score_block(i, before):
        q_val = q[pl.ds(pl.multiple_of(i * blk, blk), blk), :]
        for c in range(n_chunk):
            if c == 2 and before is not None:
                before()
            score_chunk(q_val, c)
        for r in range(BLOCK_ROWS):
            rows = slice(r * width, (r + 1) * width)
            top = jnp.max(m_buf[0, rows, :], axis=1, keepdims=True) * exp_scale
            m_buf[1, rows, :] = jnp.broadcast_to(top, (width, LANES))

    def weigh_block(more):
        for r in range(BLOCK_ROWS):
            rows = slice(r * width, (r + 1) * width)
            inv = 1.0 / jnp.sum(l_buf[rows, :], axis=1, keepdims=True)
            m_buf[2, rows, :] = jnp.broadcast_to(inv, (width, LANES))
        tot = None
        for c in range(n_chunk):
            cols = slice(c * kv_chunk, (c + 1) * kv_chunk)
            part = jnp.dot(p_buf[:, cols], v[cols, :], preferred_element_type=F32)
            tot = part if tot is None else tot + part
            if more:
                prob_chunk(c)
        o_raw[...] = tot

    def scale_o():
        for r in range(BLOCK_ROWS):
            rows = slice(r * width, (r + 1) * width)
            for col in range(0, chan, LANES):
                o_buf[rows, col:col + LANES] = (o_raw[rows, col:col + LANES] * m_buf[2, rows, :]).astype(BF16)

    def attention():
        for copy in attn_copies:
            copy.wait()
        lax.fori_loop(0, n_blk, project, 0)
        zero_stats()
        o_raw[...] = jnp.zeros_like(o_raw)
        m_buf[2] = jnp.zeros((blk, LANES), F32)
        score_block(0, None)

        @pl.when(me >= 0)
        def _():
            for c in range(n_chunk):
                prob_chunk(c)

        def step(i, carry):
            @pl.when(me >= 0)
            def _():
                scale_o()
                score_block(i + 1, lambda: out_project(i - 1, i > 0))

            weigh_block(True)
            return carry

        lax.fori_loop(0, n_blk - 1, step, 0)
        scale_o()
        out_project(n_blk - 2, None)
        weigh_block(False)
        scale_o()
        out_project(n_blk - 1, None)

    def stage(r, carry):
        set_coefs(3 * r, 0.5)
        conv_pass(h, t, 2 * r, False, 0, n_blk // 2)
        set_coefs(3 * r + 1, 0.5)

        @pl.when(r == 1)
        def _():
            for copy in keep:
                copy.start()

        last = r == 1
        conv_pass(t, h, 2 * r + 1, True, jnp.where(last, far_row, 0), jnp.where(last, n_blk // 4, n_blk // 2))

        @pl.when(r == 0)
        def _():
            set_coefs(2, 1.0)
            attention()

        return carry

    keep = [
        pltpu.make_async_copy(t, t_out, sems.at[10]),
        pltpu.make_async_copy(h.at[pl.ds(own_row, half)], h_out, sems.at[11]),
        pltpu.make_async_copy(coef, coef_out, sems.at[12]),
    ]
    lax.fori_loop(0, 2, stage, 0)

    copies = [
        pltpu.make_async_copy(h.at[pl.ds(lax.rem(me + n_dev // 2, n_dev) * band, band)], far_out, sems.at[13]),
        pltpu.make_async_copy(h.at[pl.ds((n_dev - 1 - me) * band, band)], cross_out, sems.at[14]),
    ]
    for copy in copies:
        copy.start()
    for copy in keep + copies:
        copy.wait()


def activate_row(src, row, coef, buf, r, live):
    width, chan = src.shape[1], src.shape[2]
    rows = BLOCK_ROWS + 2
    sub = lax.broadcasted_iota(jnp.int32, (8, LANES), 0)
    for col in range(0, chan, LANES):
        gain = coef[0, 0:1, col:col + LANES]
        shift = coef[1, 0:1, col:col + LANES]
        z = src[row, :, col:col + LANES].astype(F32) * gain + shift
        u = z + z * jnp.tanh(z)
        if live is not None:
            u = jnp.where(live, u, 0.0)
        left = pltpu.roll(u, 1, 0)
        left = jnp.concatenate([jnp.where(sub == 0, 0.0, left[:8]), left[8:]], axis=0)
        right = pltpu.roll(u, width - 1, 0)
        right = jnp.concatenate([right[:-8], jnp.where(sub == 7, 0.0, right[-8:])], axis=0)
        for dx, val in enumerate((left, u, right)):
            first = (dx * rows + r) * width
            buf[first:first + width, col:col + LANES] = val.astype(BF16)


def dots_of(buf, w, acc):
    chan = buf.shape[1]
    rows = BLOCK_ROWS + 2
    width = buf.shape[0] // (3 * rows)
    tot = None
    for dy in range(3):
        for dx in range(3):
            first = (dx * rows + dy) * width
            tap = (3 * dy + dx) * chan
            part = jnp.dot(buf[first:first + BLOCK_ROWS * width, :], w[tap:tap + chan, :], preferred_element_type=F32)
            tot = part if tot is None else tot + part
    acc[...] = tot


def run_sample(sample, me, x, w_in, b_in, w_conv, b_conv, gn_scale, gn_shift, w_attn, w_key, b_attn, b_key, n_dev, n_rows, width):
    chan = w_in.shape[1]
    tokens = n_rows * width
    blk = BLOCK_ROWS * width
    vmem = pl.BlockSpec(memory_space=pltpu.VMEM)
    hbm = pl.BlockSpec(memory_space=pl.ANY)
    flops = 2 * tokens * (7 * 9 * chan * chan // 2 + 4 * chan * chan + 2 * tokens * chan)
    band = jax.ShapeDtypeStruct((n_rows // n_dev, width, chan), BF16)
    return pl.pallas_call(
        functools.partial(sample_kernel, sample),
        out_shape=[
            band,
            band,
            jax.ShapeDtypeStruct((n_rows, width, chan), BF16),
            jax.ShapeDtypeStruct((n_rows // 2, width, chan), BF16),
            jax.ShapeDtypeStruct((2, 8, chan), F32),
        ],
        in_specs=[pl.BlockSpec(memory_space=pltpu.SMEM), hbm, vmem, vmem, hbm, vmem, vmem, vmem, hbm, hbm, vmem, vmem],
        out_specs=[hbm] * 5,
        scratch_shapes=[
            pltpu.VMEM(w_conv.shape, BF16),
            pltpu.VMEM(w_attn.shape, BF16),
            pltpu.VMEM((n_rows, width, chan), BF16),
            pltpu.VMEM((n_rows, width, chan), BF16),
            pltpu.VMEM((chan, tokens), BF16),
            pltpu.VMEM((tokens, chan), BF16),
            pltpu.VMEM((blk, tokens), F32),
            pltpu.VMEM((blk, tokens), BF16),
            pltpu.VMEM((blk, chan), BF16),
            pltpu.VMEM((blk, chan), F32),
            pltpu.VMEM((3, blk, LANES), F32),
            pltpu.VMEM((blk, LANES), F32),
            pltpu.VMEM((4, 8, chan), F32),
            pltpu.VMEM((4, 5, 1, chan), F32),
            pltpu.SemaphoreType.DMA((15,)),
        ],
        compiler_params=pltpu.CompilerParams(vmem_limit_bytes=67_043_328),
        cost_estimate=pl.CostEstimate(flops=flops, bytes_accessed=40 << 20, transcendentals=tokens * tokens),
        name='sample_block',
    )(me, x, w_in, b_in, w_conv, b_conv, gn_scale, gn_shift, w_attn, w_key, b_attn, b_key)


def last_kernel(n_own, n_dev, me_ref, w_hbm, b_ref, *rest):
    kept = [rest[3 * s:3 * s + 3] for s in range(n_own)]
    rest = rest[3 * n_own:]
    n_early = 2 * (n_own - 1)
    early = rest[:n_early]
    out, near_out, w, tb, hb, coefs, buf_a, buf_b, acc, staged, bias, sems = rest[n_early:]
    n_rows, width, chan = kept[0][0].shape
    band = n_rows // n_dev
    span = tb.shape[1]
    n_job = 2 * n_own
    me = me_ref[0]
    near = me + 1 - 2 * lax.rem(me, 2)
    acc_a, acc_b = acc.at[:, 0:chan], acc.at[:, chan:2 * chan]

    def band_of(k):
        return jnp.where(k < n_own, near, me)

    def first_row(k):
        return jnp.clip(band_of(k) * band - 1, 0, n_rows - span)

    w_copy = pltpu.make_async_copy(w_hbm.at[3], w, sems.at[0])
    loads = []
    for k in range(n_job):
        t_hbm, h_hbm, coef_hbm = kept[k % n_own]
        own_row = (me // (n_dev // 2)) * (n_rows // 2)
        loads.append(pltpu.make_async_copy(t_hbm.at[pl.ds(first_row(k), span)], tb.at[k], sems.at[1 + k]))
        loads.append(pltpu.make_async_copy(h_hbm.at[pl.ds(band_of(k) * band - own_row, band)], hb.at[k], sems.at[1 + n_job + k]))
        if k < n_own:
            loads.append(pltpu.make_async_copy(coef_hbm, coefs.at[k], sems.at[1 + 3 * n_job + k]))
    loads[0].start()
    loads[2].start()
    w_copy.start()
    for i, load in enumerate(loads):
        if i not in (0, 2):
            load.start()
    early_in, early_out = [], []
    for i, piece in enumerate(early):
        s, d = divmod(i, 2)
        owner = (n_dev - 1 - me) if d else lax.rem(me + n_dev // 2, n_dev)
        base = 1 + 4 * n_job
        early_in.append(pltpu.make_async_copy(piece, staged.at[i], sems.at[base + i]))
        early_out.append(pltpu.make_async_copy(staged.at[i], out.at[owner * n_own + s], sems.at[base + n_early + i]))
    for copy in early_in:
        copy.start()
    bias[...] = b_ref[3:4, :].astype(F32)

    def store_near(k):
        return pltpu.make_async_copy(hb.at[k], near_out.at[k], sems.at[1 + 2 * n_job + k])

    def store_own(k):
        return pltpu.make_async_copy(hb.at[k], out.at[me * n_own + (k - n_own)], sems.at[1 + 2 * n_job + k])

    def prep(k, b, buf):
        for r in range(BLOCK_ROWS + 2):
            row = band_of(k) * band + (b * BLOCK_ROWS + r - 1)
            row_c = jnp.clip(row, 0, n_rows - 1) - first_row(k)
            live = (row >= 0) & (row < n_rows) if r in (0, BLOCK_ROWS + 1) else None
            activate_row(tb.at[k], row_c, coefs.at[lax.rem(k, n_own)], buf, r, live)

    def finish(k, b, part, live):
        k = jnp.maximum(k, 0)
        for col in range(0, chan, LANES):
            for r in range(BLOCK_ROWS):
                row = b * BLOCK_ROWS + r
                old = hb[k, row, :, col:col + LANES].astype(F32)
                val = old + (part[r * width:(r + 1) * width, col:col + LANES] + bias[0:1, col:col + LANES])
                if live is not None:
                    val = jnp.where(live, val, old)
                hb[k, row, :, col:col + LANES] = val.astype(BF16)

    loads[0].wait()
    loads[2].wait()
    prep(jnp.int32(0), 0, buf_a)
    w_copy.wait()
    for i, load in enumerate(loads):
        if i not in (0, 2):
            load.wait()

    def job(k, carry):
        @pl.when((k >= 2) & (k < n_own + 2))
        def _():
            store_near(k - 2).start()

        @pl.when(k >= n_own + 2)
        def _():
            store_own(k - 2).start()

        @pl.when(k == 2)
        def _():
            for load, store in zip(early_in, early_out):
                load.wait()
                store.start()

        dots_of(buf_a, w, acc_a)
        prep(k, 1, buf_b)
        finish(k - 1, 1, acc_b, k > 0)
        dots_of(buf_b, w, acc_b)
        prep(jnp.minimum(k + 1, n_job - 1), 0, buf_a)
        finish(k, 0, acc_a, None)
        return carry

    lax.fori_loop(0, n_job, job, 0)
    finish(jnp.int32(n_job - 1), 1, acc_b, None)
    store_own(n_job - 2).start()
    store_own(n_job - 1).start()
    for store in early_out:
        store.wait()
    for k in range(n_job):
        (store_near if k < n_own else store_own)(k).wait()


def run_last(me, w_conv, b_conv, kept, early, n_dev, out_shape):
    n_own = len(kept)
    n_rows, width, chan = kept[0][0].shape
    band = n_rows // n_dev
    blk = BLOCK_ROWS * width
    n_job = 2 * n_own
    vmem = pl.BlockSpec(memory_space=pltpu.VMEM)
    hbm = pl.BlockSpec(memory_space=pl.ANY)
    args = [ref for refs in kept for ref in refs] + list(early)
    return pl.pallas_call(
        functools.partial(last_kernel, n_own, n_dev),
        out_shape=[jax.ShapeDtypeStruct(out_shape, BF16), jax.ShapeDtypeStruct((n_own, band, width, chan), BF16)],
        in_specs=[pl.BlockSpec(memory_space=pltpu.SMEM), hbm, vmem] + [hbm] * len(args),
        out_specs=[hbm, hbm],
        scratch_shapes=[
            pltpu.VMEM(w_conv.shape[1:], BF16),
            pltpu.VMEM((n_job, band + 2, width, chan), BF16),
            pltpu.VMEM((n_job, band, width, chan), BF16),
            pltpu.VMEM((n_own, 2, 8, chan), F32),
            pltpu.VMEM((3 * (BLOCK_ROWS + 2) * width, chan), BF16),
            pltpu.VMEM((3 * (BLOCK_ROWS + 2) * width, chan), BF16),
            pltpu.VMEM((blk, 2 * chan), F32),
            pltpu.VMEM((len(early), band, width, chan), BF16),
            pltpu.VMEM((1, chan), F32),
            pltpu.SemaphoreType.DMA((1 + 4 * n_job + 2 * len(early),)),
        ],
        compiler_params=pltpu.CompilerParams(vmem_limit_bytes=67_043_328),
        cost_estimate=pl.CostEstimate(flops=2 * n_job * band * width * 9 * chan * chan, bytes_accessed=40 << 20, transcendentals=0),
        name='last_conv',
    )(me, w_conv, b_conv, *args)


def place_kernel(n_own, n_dev, me_ref, near_ref, far_ref, cross_ref, base_ref, out, stage, in_sems, out_sems):
    del base_ref
    me = me_ref[0]
    near = me + 1 - 2 * lax.rem(me, 2)
    moves = [(near_ref.at[s], near * n_own + s) for s in range(n_own)]
    moves.append((far_ref, lax.rem(me + n_dev // 2, n_dev) * n_own + (n_own - 1)))
    moves.append((cross_ref, (n_dev - 1 - me) * n_own + (n_own - 1)))
    loads = [pltpu.make_async_copy(src, stage.at[i], in_sems.at[i]) for i, (src, _) in enumerate(moves)]
    stores = [pltpu.make_async_copy(stage.at[i], out.at[at], out_sems.at[i]) for i, (_, at) in enumerate(moves)]
    for load in loads:
        load.start()
    for load, store in zip(loads, stores):
        load.wait()
        store.start()
    for store in stores:
        store.wait()


def place(me, near, far, cross, base, n_dev):
    n_own = near.shape[0]
    hbm = pl.BlockSpec(memory_space=pl.ANY)
    n_move = n_own + 2
    return pl.pallas_call(
        functools.partial(place_kernel, n_own, n_dev),
        out_shape=jax.ShapeDtypeStruct(base.shape, BF16),
        in_specs=[pl.BlockSpec(memory_space=pltpu.SMEM)] + [hbm] * 4,
        out_specs=hbm,
        input_output_aliases={4: 0},
        scratch_shapes=[
            pltpu.VMEM((n_move,) + tuple(far.shape), BF16),
            pltpu.SemaphoreType.DMA((n_move,)),
            pltpu.SemaphoreType.DMA((n_move,)),
        ],
        cost_estimate=pl.CostEstimate(flops=1 << 20, bytes_accessed=n_move << 21, transcendentals=0),
        name='place_bands',
    )(me, near, far, cross, base)


def solution(mesh):
    n_dev = mesh.shape['cp']

    def local_fn(latents, w_in, b_in, w_conv, b_conv, gn_scale, gn_shift, w_attn, b_attn):
        me = lax.axis_index('cp').astype(jnp.int32).reshape(1)
        lat = lax.all_to_all(latents, 'cp', split_axis=0, concat_axis=1, tiled=True)
        n_own, n_rows, width, n_lat = lat.shape
        chan = w_in.shape[-1]
        tokens = n_rows * width
        flat = jnp.transpose(lat.reshape(n_own, tokens, n_lat), (0, 2, 1))
        flat = jnp.pad(flat, ((0, 0), (0, 0), (width + 1, width + 1)))
        col_pos = lax.broadcasted_iota(jnp.int32, (1, 1, tokens), 2) % width
        taps = []
        for dy in range(3):
            for dx in range(3):
                tap = flat[:, :, dy * width + dx:dy * width + dx + tokens]
                if dx == 0:
                    tap = jnp.where(col_pos == 0, jnp.zeros_like(tap), tap)
                if dx == 2:
                    tap = jnp.where(col_pos == width - 1, jnp.zeros_like(tap), tap)
                taps.append(tap)
        cols = jnp.concatenate(taps, axis=1)
        w_in2 = w_in.reshape(9 * n_lat, chan)
        w_conv2 = w_conv.reshape(4, 9 * chan, chan)
        w_key = w_attn[1].T
        b_key = b_attn[1].astype(F32).reshape(chan, 1)
        b_in2 = b_in.astype(F32).reshape(1, chan)
        out_shape = (n_own * n_dev, n_rows // n_dev, width, chan)
        kept, moved = [], []
        for s in range(n_own):
            far, cross, *keep = run_sample(s, me, cols, w_in2, b_in2, w_conv2, b_conv, gn_scale, gn_shift, w_attn, w_key,
                                           b_attn, b_key, n_dev, n_rows, width)
            kept.append(keep)
            moved.append(lax.ppermute(far, 'cp', [(j, (j + n_dev // 2) % n_dev) for j in range(n_dev)]))
            moved.append(lax.ppermute(cross, 'cp', [(j, n_dev - 1 - j) for j in range(n_dev)]))
        out, near = run_last(me, w_conv2, b_conv, kept, moved[:-2], n_dev, out_shape)
        near = lax.ppermute(near, 'cp', [(j, j ^ 1) for j in range(n_dev)])
        return place(me, near, moved[-2], moved[-1], out, n_dev)

    band_spec = P('dp', 'cp')
    whole_spec = P()
    return jax.shard_map(local_fn, mesh=mesh, in_specs=(band_spec,) + (whole_spec,) * 8, out_specs=band_spec, check_vma=False)
```

```python
import functools

import jax
import jax.numpy as jnp
import numpy as np
from jax import lax
from jax.experimental import pallas as pl
from jax.experimental.pallas import tpu as pltpu
from jax.sharding import PartitionSpec as P


GROUPS = 32
GN_EPS = 1e-6
LANES = 128
BLOCK_ROWS = 8
F32 = jnp.float32
BF16 = jnp.bfloat16


def sample_kernel(sample, me_ref, x_hbm, w_in_ref, b_in_ref, w_conv_hbm, b_conv_ref, gn_scale_ref, gn_shift_ref,
                  w_attn_hbm, w_key_hbm, b_attn_ref, b_key_ref, far_out, cross_out, t_out, h_out, coef_out,
                  w_conv, w_attn, h, t, kt, v, s_buf, p_buf, o_buf, o_raw, m_buf, l_buf, small, params, sems):
    n_dev = h.shape[0] // far_out.shape[0]
    n_rows, width, chan = h.shape
    tokens = n_rows * width
    blk = BLOCK_ROWS * width
    n_blk = n_rows // BLOCK_ROWS
    count = tokens * (chan // GROUPS)
    n_cols = w_in_ref.shape[0]
    stat, coef = small.at[0:2], small.at[2:4]
    acc_a, acc_b = s_buf.at[:, 0:chan], s_buf.at[:, chan:2 * chan]
    lhs_rows = 3 * (BLOCK_ROWS + 2) * width
    buf_a, buf_b = v.at[0:lhs_rows], v.at[tokens // 2:tokens // 2 + lhs_rows]

    def conv_copy(idx):
        return pltpu.make_async_copy(w_conv_hbm.at[idx], w_conv.at[idx], sems.at[idx])

    attn_copies = [pltpu.make_async_copy(w_key_hbm if i == 1 else w_attn_hbm.at[i], w_attn.at[i], sems.at[6 + i]) for i in range(4)]
    me = me_ref[0]
    band = n_rows // n_dev
    half = n_rows // 2
    own_row = (me // (n_dev // 2)) * half
    far_row = half - own_row
    for i, ref in enumerate((gn_scale_ref, gn_shift_ref, b_conv_ref, b_attn_ref)):
        val = ref[...].astype(F32)
        for k in range(val.shape[0]):
            params[i, k] = val[k:k + 1]
    gn_scale, gn_shift, b_conv, b_attn = (params.at[i] for i in range(4))
    x_copy = pltpu.make_async_copy(x_hbm.at[sample], p_buf.at[0:n_cols, :], sems.at[5])
    x_copy.start()
    conv_copy(0).start()

    def zero_stats():
        stat[...] = jnp.zeros((2, 8, chan), F32)

    def finish(get, put, live):
        for col in range(0, chan, LANES):
            tot = jnp.zeros((8, LANES), F32)
            tot_sq = jnp.zeros((8, LANES), F32)
            for r in range(BLOCK_ROWS):
                val = get(r, col).astype(BF16)
                put(r, col, val)
                val = val.astype(F32).reshape(width // 8, 8, LANES)
                tot = tot + jnp.sum(val, axis=0)
                tot_sq = tot_sq + jnp.sum(val * val, axis=0)
            if live is not None:
                tot = jnp.where(live, tot, 0.0)
                tot_sq = jnp.where(live, tot_sq, 0.0)
            stat[0, :, col:col + LANES] += tot
            stat[1, :, col:col + LANES] += tot_sq

    def set_coefs(idx, half):
        lane = lax.broadcasted_iota(jnp.int32, (8, chan), 1)

        def group_sum(part):
            tot = jnp.broadcast_to(jnp.sum(part, axis=0, keepdims=True), (8, chan))
            for step in (1, 2, 4, 8):
                above = pltpu.roll(tot, chan - step, 1)
                below = pltpu.roll(tot, step, 1)
                tot = tot + jnp.where((lane & step) == 0, above, below)
            return tot

        mean = group_sum(stat[0]) * (1.0 / count)
        var = jnp.maximum(group_sum(stat[1]) * (1.0 / count) - mean * mean, 0.0)
        gain = gn_scale[idx] * lax.rsqrt(var + GN_EPS)
        shift = gn_shift[idx] - mean * gain
        coef[0] = gain * half
        coef[1] = shift * half

    zero_stats()

    def conv_in_step(b, carry):
        lhs = p_buf[0:n_cols, pl.ds(pl.multiple_of(b * blk, blk), blk)]
        acc_a[...] = lax.dot_general(lhs, w_in_ref[...], (((0,), (0,)), ((), ())), preferred_element_type=F32)

        def get(r, col):
            return acc_a[r * width:(r + 1) * width, col:col + LANES] + b_in_ref[0:1, col:col + LANES]

        def put(r, col, val):
            h[b * BLOCK_ROWS + r, :, col:col + LANES] = val

        finish(get, put, None)
        return carry

    x_copy.wait()
    lax.fori_loop(0, n_blk, conv_in_step, 0)

    def prep(src, buf, b, base):
        for r in range(BLOCK_ROWS + 2):
            row = base + b * BLOCK_ROWS + (r - 1)
            row_c = jnp.clip(row, 0, n_rows - 1)
            live = (row >= 0) & (row < n_rows) if r in (0, BLOCK_ROWS + 1) else None
            activate_row(src, row_c, coef, buf, r, live)

    def conv_dots(buf, acc, idx):
        dots_of(buf, w_conv.at[idx], acc)

    def conv_finish(acc, dst, idx, b, base, residual, live):
        row0 = base + jnp.maximum(b, 0) * BLOCK_ROWS

        def get(r, col):
            val = acc[r * width:(r + 1) * width, col:col + LANES] + b_conv[idx, 0:1, col:col + LANES]
            if residual:
                old = dst[row0 + r, :, col:col + LANES].astype(F32)
                val = old + val
                if live is not None:
                    val = jnp.where(live, val, old)
            return val

        def put(r, col, val):
            dst[row0 + r, :, col:col + LANES] = val

        finish(get, put, live)

    def conv_pass(src, dst, idx, residual, base, pairs):
        zero_stats()
        prep(src, buf_a, 0, base)
        conv_copy(idx).wait()
        if not residual:
            @pl.when(idx == 0)
            def _():
                for copy in [conv_copy(1)] + attn_copies + [conv_copy(2), conv_copy(3)]:
                    copy.start()

        def pair(j, carry):
            conv_dots(buf_a, acc_a, idx)
            prep(src, buf_b, 2 * j + 1, base)
            conv_finish(acc_b, dst, idx, 2 * j - 1, base, residual, j > 0)
            conv_dots(buf_b, acc_b, idx)
            prep(src, buf_a, 2 * j + 2, base)
            conv_finish(acc_a, dst, idx, 2 * j, base, residual, None)
            return carry

        lax.fori_loop(0, pairs, pair, 0)
        conv_finish(acc_b, dst, idx, 2 * pairs - 1, base, residual, None)

    q = t.reshape(tokens, chan)
    kv_chunk = 512
    n_chunk = tokens // kv_chunk
    exp_scale = float(chan ** -0.5 * np.log2(np.e))

    def project(b, carry):
        norm = h[pl.ds(b * BLOCK_ROWS, BLOCK_ROWS)].reshape(blk, chan).astype(F32) * coef[0, 0:1, :] + coef[1, 0:1, :]
        norm = norm.astype(BF16)
        rows = pl.ds(pl.multiple_of(b * blk, blk), blk)
        q[rows, :] = (jnp.dot(norm, w_attn[0], preferred_element_type=F32) + b_attn[0]).astype(BF16)
        v[rows, :] = (jnp.dot(norm, w_attn[2], preferred_element_type=F32) + b_attn[2]).astype(BF16)
        keys = lax.dot_general(w_attn[1], norm, (((1,), (1,)), ((), ())), preferred_element_type=F32)
        kt[:, pl.ds(pl.multiple_of(b * blk, blk), blk)] = (keys + b_key_ref[...]).astype(BF16)
        return carry

    def score_chunk(q_val, c):
        val = jnp.dot(q_val, kt[:, c * kv_chunk:(c + 1) * kv_chunk], preferred_element_type=F32)
        s_buf[:, c * kv_chunk:(c + 1) * kv_chunk] = val
        for r in range(BLOCK_ROWS):
            rows = slice(r * width, (r + 1) * width)
            top = val[rows, 0:LANES]
            for col in range(LANES, kv_chunk, LANES):
                top = jnp.maximum(top, val[rows, col:col + LANES])
            m_buf[0, rows, :] = top if c == 0 else jnp.maximum(m_buf[0, rows, :], top)

    def prob_chunk(c):
        for r in range(BLOCK_ROWS):
            rows = slice(r * width, (r + 1) * width)
            m_scaled = m_buf[1, rows, :]
            tot = None
            for col in range(c * kv_chunk, (c + 1) * kv_chunk, LANES):
                val = jnp.exp2(s_buf[rows, col:col + LANES] * exp_scale - m_scaled)
                p_buf[rows, col:col + LANES] = val.astype(BF16)
                tot = val if tot is None else tot + val
            l_buf[rows, :] = tot if c == 0 else l_buf[rows, :] + tot

    def out_project(b, live):
        row0 = jnp.maximum(b, 0) * BLOCK_ROWS
        prod = jnp.dot(o_buf[...], w_attn[3], preferred_element_type=F32)

        def get(r, col):
            old = h[row0 + r, :, col:col + LANES].astype(F32)
            val = old + (prod[r * width:(r + 1) * width, col:col + LANES] + b_attn[3, 0:1, col:col + LANES])
            return val if live is None else jnp.where(live, val, old)

        def put(r, col, val):
            h[row0 + r, :, col:col + LANES] = val

        finish(get, put, live)

    def score_block(i, before):
        q_val = q[pl.ds(pl.multiple_of(i * blk, blk), blk), :]
        for c in range(n_chunk):
            if c == 2 and before is not None:
                before()
            score_chunk(q_val, c)
        for r in range(BLOCK_ROWS):
            rows = slice(r * width, (r + 1) * width)
            top = jnp.max(m_buf[0, rows, :], axis=1, keepdims=True) * exp_scale
            m_buf[1, rows, :] = jnp.broadcast_to(top, (width, LANES))

    def weigh_block(more):
        for r in range(BLOCK_ROWS):
            rows = slice(r * width, (r + 1) * width)
            inv = 1.0 / jnp.sum(l_buf[rows, :], axis=1, keepdims=True)
            m_buf[2, rows, :] = jnp.broadcast_to(inv, (width, LANES))
        tot = None
        for c in range(n_chunk):
            cols = slice(c * kv_chunk, (c + 1) * kv_chunk)
            part = jnp.dot(p_buf[:, cols], v[cols, :], preferred_element_type=F32)
            tot = part if tot is None else tot + part
            if more:
                prob_chunk(c)
        o_raw[...] = tot

    def scale_o():
        for r in range(BLOCK_ROWS):
            rows = slice(r * width, (r + 1) * width)
            for col in range(0, chan, LANES):
                o_buf[rows, col:col + LANES] = (o_raw[rows, col:col + LANES] * m_buf[2, rows, :]).astype(BF16)

    def attention():
        for copy in attn_copies:
            copy.wait()
        lax.fori_loop(0, n_blk, project, 0)
        zero_stats()
        o_raw[...] = jnp.zeros_like(o_raw)
        m_buf[2] = jnp.zeros((blk, LANES), F32)
        score_block(0, None)

        @pl.when(me >= 0)
        def _():
            for c in range(n_chunk):
                prob_chunk(c)

        def step(i, carry):
            @pl.when(me >= 0)
            def _():
                scale_o()
                score_block(i + 1, lambda: out_project(i - 1, i > 0))

            weigh_block(True)
            return carry

        lax.fori_loop(0, n_blk - 1, step, 0)
        scale_o()
        out_project(n_blk - 2, None)
        weigh_block(False)
        scale_o()
        out_project(n_blk - 1, None)

    def stage(r, carry):
        set_coefs(3 * r, 0.5)
        conv_pass(h, t, 2 * r, False, 0, n_blk // 2)
        set_coefs(3 * r + 1, 0.5)

        @pl.when(r == 1)
        def _():
            for copy in keep:
                copy.start()

        last = r == 1
        conv_pass(t, h, 2 * r + 1, True, jnp.where(last, far_row, 0), jnp.where(last, n_blk // 4, n_blk // 2))

        @pl.when(r == 0)
        def _():
            set_coefs(2, 1.0)
            attention()

        return carry

    keep = [
        pltpu.make_async_copy(t, t_out, sems.at[10]),
        pltpu.make_async_copy(h.at[pl.ds(own_row, half)], h_out, sems.at[11]),
        pltpu.make_async_copy(coef, coef_out, sems.at[12]),
    ]
    lax.fori_loop(0, 2, stage, 0)

    copies = [
        pltpu.make_async_copy(h.at[pl.ds(lax.rem(me + n_dev // 2, n_dev) * band, band)], far_out, sems.at[13]),
        pltpu.make_async_copy(h.at[pl.ds((n_dev - 1 - me) * band, band)], cross_out, sems.at[14]),
    ]
    for copy in copies:
        copy.start()
    for copy in keep + copies:
        copy.wait()


def activate_row(src, row, coef, buf, r, live):
    width, chan = src.shape[1], src.shape[2]
    rows = BLOCK_ROWS + 2
    sub = lax.broadcasted_iota(jnp.int32, (8, LANES), 0)
    for col in range(0, chan, LANES):
        gain = coef[0, 0:1, col:col + LANES]
        shift = coef[1, 0:1, col:col + LANES]
        z = src[row, :, col:col + LANES].astype(F32) * gain + shift
        u = z + z * jnp.tanh(z)
        if live is not None:
            u = jnp.where(live, u, 0.0)
        left = pltpu.roll(u, 1, 0)
        left = jnp.concatenate([jnp.where(sub == 0, 0.0, left[:8]), left[8:]], axis=0)
        right = pltpu.roll(u, width - 1, 0)
        right = jnp.concatenate([right[:-8], jnp.where(sub == 7, 0.0, right[-8:])], axis=0)
        for dx, val in enumerate((left, u, right)):
            first = (dx * rows + r) * width
            buf[first:first + width, col:col + LANES] = val.astype(BF16)


def dots_of(buf, w, acc):
    chan = buf.shape[1]
    rows = BLOCK_ROWS + 2
    width = buf.shape[0] // (3 * rows)
    tot = None
    for dy in range(3):
        for dx in range(3):
            first = (dx * rows + dy) * width
            tap = (3 * dy + dx) * chan
            part = jnp.dot(buf[first:first + BLOCK_ROWS * width, :], w[tap:tap + chan, :], preferred_element_type=F32)
            tot = part if tot is None else tot + part
    acc[...] = tot


def run_sample(sample, me, x, w_in, b_in, w_conv, b_conv, gn_scale, gn_shift, w_attn, w_key, b_attn, b_key, n_dev, n_rows, width):
    chan = w_in.shape[1]
    tokens = n_rows * width
    blk = BLOCK_ROWS * width
    vmem = pl.BlockSpec(memory_space=pltpu.VMEM)
    hbm = pl.BlockSpec(memory_space=pl.ANY)
    flops = 2 * tokens * (7 * 9 * chan * chan // 2 + 4 * chan * chan + 2 * tokens * chan)
    band = jax.ShapeDtypeStruct((n_rows // n_dev, width, chan), BF16)
    return pl.pallas_call(
        functools.partial(sample_kernel, sample),
        out_shape=[
            band,
            band,
            jax.ShapeDtypeStruct((n_rows, width, chan), BF16),
            jax.ShapeDtypeStruct((n_rows // 2, width, chan), BF16),
            jax.ShapeDtypeStruct((2, 8, chan), F32),
        ],
        in_specs=[pl.BlockSpec(memory_space=pltpu.SMEM), hbm, vmem, vmem, hbm, vmem, vmem, vmem, hbm, hbm, vmem, vmem],
        out_specs=[hbm] * 5,
        scratch_shapes=[
            pltpu.VMEM(w_conv.shape, BF16),
            pltpu.VMEM(w_attn.shape, BF16),
            pltpu.VMEM((n_rows, width, chan), BF16),
            pltpu.VMEM((n_rows, width, chan), BF16),
            pltpu.VMEM((chan, tokens), BF16),
            pltpu.VMEM((tokens, chan), BF16),
            pltpu.VMEM((blk, tokens), F32),
            pltpu.VMEM((blk, tokens), BF16),
            pltpu.VMEM((blk, chan), BF16),
            pltpu.VMEM((blk, chan), F32),
            pltpu.VMEM((3, blk, LANES), F32),
            pltpu.VMEM((blk, LANES), F32),
            pltpu.VMEM((4, 8, chan), F32),
            pltpu.VMEM((4, 5, 1, chan), F32),
            pltpu.SemaphoreType.DMA((15,)),
        ],
        compiler_params=pltpu.CompilerParams(vmem_limit_bytes=67_043_328),
        cost_estimate=pl.CostEstimate(flops=flops, bytes_accessed=40 << 20, transcendentals=tokens * tokens),
        name='sample_block',
    )(me, x, w_in, b_in, w_conv, b_conv, gn_scale, gn_shift, w_attn, w_key, b_attn, b_key)


def last_kernel(n_own, n_dev, me_ref, w_hbm, b_ref, *rest):
    kept = [rest[3 * s:3 * s + 3] for s in range(n_own)]
    rest = rest[3 * n_own:]
    n_early = 2 * (n_own - 1)
    early = rest[:n_early]
    out, near_out, w, tb, hb, coefs, buf_a, buf_b, acc, staged, bias, sems = rest[n_early:]
    n_rows, width, chan = kept[0][0].shape
    band = n_rows // n_dev
    span = tb.shape[1]
    n_job = 2 * n_own
    me = me_ref[0]
    near = me + 1 - 2 * lax.rem(me, 2)
    acc_a, acc_b = acc.at[:, 0:chan], acc.at[:, chan:2 * chan]

    def band_of(k):
        return jnp.where(k < n_own, near, me)

    def first_row(k):
        return jnp.clip(band_of(k) * band - 1, 0, n_rows - span)

    w_copy = pltpu.make_async_copy(w_hbm.at[3], w, sems.at[0])
    loads = []
    for k in range(n_job):
        t_hbm, h_hbm, coef_hbm = kept[k % n_own]
        own_row = (me // (n_dev // 2)) * (n_rows // 2)
        loads.append(pltpu.make_async_copy(t_hbm.at[pl.ds(first_row(k), span)], tb.at[k], sems.at[1 + k]))
        loads.append(pltpu.make_async_copy(h_hbm.at[pl.ds(band_of(k) * band - own_row, band)], hb.at[k], sems.at[1 + n_job + k]))
        if k < n_own:
            loads.append(pltpu.make_async_copy(coef_hbm, coefs.at[k], sems.at[1 + 3 * n_job + k]))
    first_loads, later_loads = loads[:6], loads[6:]
    w_copy.start()
    for load in first_loads:
        load.start()
    early_in, early_out = [], []
    for i, piece in enumerate(early):
        s, d = divmod(i, 2)
        owner = (n_dev - 1 - me) if d else lax.rem(me + n_dev // 2, n_dev)
        base = 1 + 4 * n_job
        early_in.append(pltpu.make_async_copy(piece, staged.at[i], sems.at[base + i]))
        early_out.append(pltpu.make_async_copy(staged.at[i], out.at[owner * n_own + s], sems.at[base + n_early + i]))
    bias[...] = b_ref[3:4, :].astype(F32)

    def store_near(k):
        return pltpu.make_async_copy(hb.at[k], near_out.at[k], sems.at[1 + 2 * n_job + k])

    def store_own(k):
        return pltpu.make_async_copy(hb.at[k], out.at[me * n_own + (k - n_own)], sems.at[1 + 2 * n_job + k])

    def prep(k, b, buf):
        for r in range(BLOCK_ROWS + 2):
            row = band_of(k) * band + (b * BLOCK_ROWS + r - 1)
            row_c = jnp.clip(row, 0, n_rows - 1) - first_row(k)
            live = (row >= 0) & (row < n_rows) if r in (0, BLOCK_ROWS + 1) else None
            activate_row(tb.at[k], row_c, coefs.at[lax.rem(k, n_own)], buf, r, live)

    def finish(k, b, part, live):
        k = jnp.maximum(k, 0)
        for col in range(0, chan, LANES):
            for r in range(BLOCK_ROWS):
                row = b * BLOCK_ROWS + r
                old = hb[k, row, :, col:col + LANES].astype(F32)
                val = old + (part[r * width:(r + 1) * width, col:col + LANES] + bias[0:1, col:col + LANES])
                if live is not None:
                    val = jnp.where(live, val, old)
                hb[k, row, :, col:col + LANES] = val.astype(BF16)

    for load in first_loads:
        load.wait()
    prep(jnp.int32(0), 0, buf_a)
    w_copy.wait()
    for load in later_loads:
        load.start()

    def job(k, carry):
        @pl.when((k >= 2) & (k < n_own + 2))
        def _():
            store_near(k - 2).start()

        @pl.when(k >= n_own + 2)
        def _():
            store_own(k - 2).start()

        @pl.when(k == 1)
        def _():
            for load in later_loads:
                load.wait()
            for load in early_in:
                load.start()

        @pl.when(k == 3)
        def _():
            for load, store in zip(early_in, early_out):
                load.wait()
                store.start()

        dots_of(buf_a, w, acc_a)
        prep(k, 1, buf_b)
        finish(k - 1, 1, acc_b, k > 0)
        dots_of(buf_b, w, acc_b)
        prep(jnp.minimum(k + 1, n_job - 1), 0, buf_a)
        finish(k, 0, acc_a, None)
        return carry

    lax.fori_loop(0, n_job, job, 0)
    finish(jnp.int32(n_job - 1), 1, acc_b, None)
    store_own(n_job - 2).start()
    store_own(n_job - 1).start()
    for store in early_out:
        store.wait()
    for k in range(n_job):
        (store_near if k < n_own else store_own)(k).wait()


def run_last(me, w_conv, b_conv, kept, early, n_dev, out_shape):
    n_own = len(kept)
    n_rows, width, chan = kept[0][0].shape
    band = n_rows // n_dev
    blk = BLOCK_ROWS * width
    n_job = 2 * n_own
    vmem = pl.BlockSpec(memory_space=pltpu.VMEM)
    hbm = pl.BlockSpec(memory_space=pl.ANY)
    args = [ref for refs in kept for ref in refs] + list(early)
    return pl.pallas_call(
        functools.partial(last_kernel, n_own, n_dev),
        out_shape=[jax.ShapeDtypeStruct(out_shape, BF16), jax.ShapeDtypeStruct((n_own, band, width, chan), BF16)],
        in_specs=[pl.BlockSpec(memory_space=pltpu.SMEM), hbm, vmem] + [hbm] * len(args),
        out_specs=[hbm, hbm],
        scratch_shapes=[
            pltpu.VMEM(w_conv.shape[1:], BF16),
            pltpu.VMEM((n_job, band + 2, width, chan), BF16),
            pltpu.VMEM((n_job, band, width, chan), BF16),
            pltpu.VMEM((n_own, 2, 8, chan), F32),
            pltpu.VMEM((3 * (BLOCK_ROWS + 2) * width, chan), BF16),
            pltpu.VMEM((3 * (BLOCK_ROWS + 2) * width, chan), BF16),
            pltpu.VMEM((blk, 2 * chan), F32),
            pltpu.VMEM((len(early), band, width, chan), BF16),
            pltpu.VMEM((1, chan), F32),
            pltpu.SemaphoreType.DMA((1 + 4 * n_job + 2 * len(early),)),
        ],
        compiler_params=pltpu.CompilerParams(vmem_limit_bytes=67_043_328),
        cost_estimate=pl.CostEstimate(flops=2 * n_job * band * width * 9 * chan * chan, bytes_accessed=40 << 20, transcendentals=0),
        name='last_conv',
    )(me, w_conv, b_conv, *args)


def place_kernel(n_own, n_dev, me_ref, near_ref, far_ref, cross_ref, base_ref, out, stage, in_sems, out_sems):
    del base_ref
    me = me_ref[0]
    near = me + 1 - 2 * lax.rem(me, 2)
    moves = [(near_ref.at[s], near * n_own + s) for s in range(n_own)]
    moves.append((far_ref, lax.rem(me + n_dev // 2, n_dev) * n_own + (n_own - 1)))
    moves.append((cross_ref, (n_dev - 1 - me) * n_own + (n_own - 1)))
    loads = [pltpu.make_async_copy(src, stage.at[i], in_sems.at[i]) for i, (src, _) in enumerate(moves)]
    stores = [pltpu.make_async_copy(stage.at[i], out.at[at], out_sems.at[i]) for i, (_, at) in enumerate(moves)]
    for load in loads:
        load.start()
    for load, store in zip(loads, stores):
        load.wait()
        store.start()
    for store in stores:
        store.wait()


def place(me, near, far, cross, base, n_dev):
    n_own = near.shape[0]
    hbm = pl.BlockSpec(memory_space=pl.ANY)
    n_move = n_own + 2
    return pl.pallas_call(
        functools.partial(place_kernel, n_own, n_dev),
        out_shape=jax.ShapeDtypeStruct(base.shape, BF16),
        in_specs=[pl.BlockSpec(memory_space=pltpu.SMEM)] + [hbm] * 4,
        out_specs=hbm,
        input_output_aliases={4: 0},
        scratch_shapes=[
            pltpu.VMEM((n_move,) + tuple(far.shape), BF16),
            pltpu.SemaphoreType.DMA((n_move,)),
            pltpu.SemaphoreType.DMA((n_move,)),
        ],
        cost_estimate=pl.CostEstimate(flops=1 << 20, bytes_accessed=n_move << 21, transcendentals=0),
        name='place_bands',
    )(me, near, far, cross, base)


def solution(mesh):
    n_dev = mesh.shape['cp']

    def local_fn(latents, w_in, b_in, w_conv, b_conv, gn_scale, gn_shift, w_attn, b_attn):
        me = lax.axis_index('cp').astype(jnp.int32).reshape(1)
        lat = lax.all_to_all(latents, 'cp', split_axis=0, concat_axis=1, tiled=True)
        n_own, n_rows, width, n_lat = lat.shape
        chan = w_in.shape[-1]
        tokens = n_rows * width
        flat = jnp.transpose(lat.reshape(n_own, tokens, n_lat), (0, 2, 1))
        flat = jnp.pad(flat, ((0, 0), (0, 0), (width + 1, width + 1)))
        col_pos = lax.broadcasted_iota(jnp.int32, (1, 1, tokens), 2) % width
        taps = []
        for dy in range(3):
            for dx in range(3):
                tap = flat[:, :, dy * width + dx:dy * width + dx + tokens]
                if dx == 0:
                    tap = jnp.where(col_pos == 0, jnp.zeros_like(tap), tap)
                if dx == 2:
                    tap = jnp.where(col_pos == width - 1, jnp.zeros_like(tap), tap)
                taps.append(tap)
        cols = jnp.concatenate(taps, axis=1)
        w_in2 = w_in.reshape(9 * n_lat, chan)
        w_conv2 = w_conv.reshape(4, 9 * chan, chan)
        w_key = w_attn[1].T
        b_key = b_attn[1].astype(F32).reshape(chan, 1)
        b_in2 = b_in.astype(F32).reshape(1, chan)
        out_shape = (n_own * n_dev, n_rows // n_dev, width, chan)
        kept, moved = [], []
        for s in range(n_own):
            far, cross, *keep = run_sample(s, me, cols, w_in2, b_in2, w_conv2, b_conv, gn_scale, gn_shift, w_attn, w_key,
                                           b_attn, b_key, n_dev, n_rows, width)
            kept.append(keep)
            moved.append(lax.ppermute(far, 'cp', [(j, (j + n_dev // 2) % n_dev) for j in range(n_dev)]))
            moved.append(lax.ppermute(cross, 'cp', [(j, n_dev - 1 - j) for j in range(n_dev)]))
        out, near = run_last(me, w_conv2, b_conv, kept, moved[:-2], n_dev, out_shape)
        near = lax.ppermute(near, 'cp', [(j, j ^ 1) for j in range(n_dev)])
        return place(me, near, moved[-2], moved[-1], out, n_dev)

    band_spec = P('dp', 'cp')
    whole_spec = P()
    return jax.shard_map(local_fn, mesh=mesh, in_specs=(band_spec,) + (whole_spec,) * 8, out_specs=band_spec, check_vma=False)
```
